256 devices in a mesh: tok: 32 (over y, z), voc: 8 (over x, core).
Axes of the slice: x: 4, y: 4, z: 8, core: 2. Of those that a mesh axis runs over, the one named last changes fastest.
Arguments:
- hidden: bfloat16 [768, 4096], P(('tok', 'voc'))
- head_weight: bfloat16 [4096, 128256], P(None, ('tok', 'voc'))
- actions: int32 [768], P(('tok', 'voc')), may hold values from 0 to 128255
- old_logp: bfloat16 [768], P(('tok', 'voc')), may hold values from -80 to 1
- advantage: bfloat16 [768], P(('tok', 'voc')), may hold values from -4 to 4
- loss_mask: int32 [768], P(('tok', 'voc')), may hold values 0 or 1
Outputs:
- grad_weight: bfloat16 [4096, 128256], P(None, ('tok', 'voc'))
- grad_hidden: float32 [768, 4096], P(('tok', 'voc'))
The draws below stay inside these ranges and needn't reach their ends.
All inputs are finite; a program needn't handle non-finite values. No bound on the sum of `loss_mask` on one device may be relied on, other than what follows from the above.
Results may differ from the reference program's by a relative error of at most 0.0047.
Values may be sent and summed in bfloat16 or wider, within the bound.
No kernel may reach another device: no remote copies, remote signals or barrier semaphores. Data moves between devices by JAX's collectives and lax.ppermute only.
A program may use at most 128 MiB of HBM per device.

```python
import jax
import jax.numpy as jnp
from jax import lax

D = 4096
VOCAB = 128256
TOKENS = 768


def unscaled_columns(key):
    wkey = jax.random.fold_in(key, 11)
    columns = jnp.arange(VOCAB)
    return jax.vmap(lambda c: jax.random.normal(jax.random.fold_in(wkey, c), (D,), jnp.float32))(columns)


def head_from(columns):
    return (jnp.transpose(columns) * (3.0 / jnp.sqrt(jnp.float32(D)))).astype(jnp.bfloat16)


def sampled_ids(key):
    return jax.random.randint(jax.random.fold_in(key, 13), (TOKENS,), 0, VOCAB).astype(jnp.int32)


def make_hidden(key, columns, chosen):
    hkey = jax.random.fold_in(key, 17)
    values = jax.random.normal(hkey, (TOKENS, D), jnp.float32)
    return values.astype(jnp.bfloat16)


def draw_head_weight(key, part):
    return head_from(unscaled_columns(key))


def draw_actions(key, part):
    return sampled_ids(key)


def draw_hidden(key, part):
    columns = unscaled_columns(key)
    return make_hidden(key, columns, sampled_ids(key))


def draw_old_logp(key, part):
    columns = unscaled_columns(key)
    chosen = sampled_ids(key)
    states = make_hidden(key, columns, chosen)
    logits = jnp.dot(states, head_from(columns), preferred_element_type=jnp.float32)
    top = jnp.max(logits, axis=1)
    lse = top + jnp.log(jnp.sum(jnp.exp(logits - top[:, None]), axis=1))
    target = jnp.take_along_axis(logits, chosen[:, None], axis=1)[:, 0]
    noise = jax.random.uniform(jax.random.fold_in(key, 19), (TOKENS,), jnp.float32, -0.5, 0.5)
    return jnp.clip(target - lse + noise, -80.0, 1.0).astype(jnp.bfloat16)


def with_ends(result, stream_key, least, top_value):
    extent = result.shape
    index_at = [jax.random.randint(jax.random.fold_in(stream_key, axis), (), 0, extent[axis]) for axis in range(len(extent))]
    result = result.at[tuple(index_at)].set(least)
    longest = extent.index(max(extent))
    index_at[longest] = (index_at[longest] + 1) % extent[longest]
    return result.at[tuple(index_at)].set(top_value)


def block_levels(key, dims, cuts, least, high):
    def one(axis_at, parts):
        heights = jax.random.uniform(jax.random.fold_in(jax.random.fold_in(key, 6), axis_at), (parts,), jnp.float32, least / len(cuts), high / len(cuts))
        return jnp.repeat(jnp.exp(heights), dims[axis_at] // parts).reshape((-1,) + (1,) * (len(dims) - axis_at - 1))

    loudness = one(*cuts[0])
    for cut in cuts[1:]:
        loudness = loudness * one(*cut)
    return loudness


def scatter_about(stream_key, dims, spread, most, split=(), held_as=jnp.bfloat16):
    factor_of = block_levels(stream_key, dims, split, -0.22, 0.18) if split else 1.0
    entries = jax.random.normal(stream_key, dims, jnp.float32) * spread * factor_of
    return jnp.minimum(jnp.maximum(entries, -most), most).astype(held_as)


def setup_inputs(seed: int = 0) -> dict:
    key_list = jax.random.split(jax.random.key(seed), 7)
    return {
        "hidden": draw_hidden(jax.random.fold_in(key_list[6], 71), 0),
        "head_weight": draw_head_weight(jax.random.fold_in(key_list[6], 71), 0),
        "actions": draw_actions(jax.random.fold_in(key_list[6], 71), 0),
        "old_logp": draw_old_logp(jax.random.fold_in(key_list[6], 71), 0),
        "advantage": scatter_about(key_list[4], (TOKENS,), 1.0, 4.0, ((0, 256),)),
        "loss_mask": with_ends((jax.random.randint(key_list[5], (TOKENS,), 0, 4) < 3).astype(jnp.int32), jax.random.fold_in(key_list[5], 1), 0, 1),
    }


def reference(hidden, head_weight, actions, old_logp, advantage, loss_mask):
    logits = jnp.dot(hidden, head_weight, preferred_element_type=jnp.float32)
    top = jnp.max(logits, axis=1)
    shifted = jnp.exp(logits - top[:, None])
    sumexp = jnp.sum(shifted, axis=1)
    moment = jnp.sum(shifted * logits, axis=1)
    target = jnp.take_along_axis(logits, actions[:, None].astype(jnp.int32), axis=1)[:, 0]
    lse = top + jnp.log(sumexp)
    mean_logit = moment / sumexp
    logp = target - lse
    advant = advantage.astype(jnp.float32)
    ratio = jnp.exp(logp - old_logp.astype(jnp.float32))
    clipped = ((advant > 0.0) & (ratio > 1.2)) | ((advant < 0.0) & (ratio < 0.8))
    active = jnp.where(clipped, 0.0, 1.0).astype(jnp.float32)
    weights = loss_mask.astype(jnp.float32)
    policy = -advant * ratio * active * weights
    probability = jnp.exp(logits - lse[:, None])
    columns = lax.broadcasted_iota(jnp.int32, logits.shape, 1)
    onehot = (columns == actions[:, None].astype(jnp.int32)).astype(jnp.float32)
    dlogits = policy[:, None] * (onehot - probability) + 0.05 * weights[:, None] * probability * (logits - mean_logit[:, None])
    dlogits = dlogits.astype(jnp.bfloat16)
    grad_weight = lax.dot_general(hidden, dlogits, (((0,), (0,)), ((), ())), preferred_element_type=jnp.float32).astype(jnp.bfloat16)
    grad_hidden = lax.dot_general(dlogits, head_weight, (((1,), (1,)), ((), ())), preferred_element_type=jnp.float32)
    return grad_weight, grad_hidden
```

```python
import jax
import jax.numpy as jnp
from jax import lax
from jax.sharding import Mesh
from jax.sharding import PartitionSpec as P

Y, Z, X, C = "tok_0", "tok_1", "voc_0", "voc_1"
TOK_VOC = (Y, Z, X, C)
NY, NZ, NX, NC = 4, 8, 4, 2
EXTRA = 128


def place(y, z, x, c):
    return ((y % NY) * NZ + z % NZ) * NX * NC + (x % NX) * NC + c % NC


def along_y(core):
    return [[place(y, z, x, core) for y in range(NY)] for z in range(NZ) for x in range(NX)]


def along_x(core):
    return [[place(y, z, x, core) for x in range(NX)] for y in range(NY) for z in range(NZ)]


LONG = along_y(0) + along_x(1)
SHORT = along_x(0) + along_y(1)
SWAP = [
    (place(y, z, x, c), place(y, z, x, 1 - c))
    for y in range(NY)
    for z in range(NZ)
    for x in range(NX)
    for c in range(NC)
]


def exchange(blocks, axis, groups=None):
    return lax.all_to_all(blocks, axis, 0, 0, axis_index_groups=groups)


def gathered(block, count, axis, groups=None):
    whole = exchange(jnp.broadcast_to(block, (count, *block.shape)), axis, groups)
    return whole.reshape(-1, *block.shape[1:])


def scattered(partial, count, axis, groups=None):
    pieces = exchange(partial.reshape(count, -1, partial.shape[1]), axis, groups)
    return jnp.sum(pieces.astype(jnp.float32), axis=0)


def combined(stats, count, axis):
    pieces = exchange(jnp.broadcast_to(stats, (count, *stats.shape)), axis)
    top = jnp.max(pieces[:, 0], axis=0)
    scale = jnp.exp(pieces[:, 0] - top)
    return jnp.stack(
        [
            top,
            jnp.sum(pieces[:, 1] * scale, axis=0),
            jnp.sum(pieces[:, 2] * scale, axis=0),
            jnp.sum(pieces[:, 3], axis=0),
        ]
    )


def per_device(hidden, head_weight, actions, old_logp, advantage, loss_mask):
    model, width = head_weight.shape
    core = lax.axis_index(C)
    digits = [actions % 128, (actions // 128) % 128, actions // 16384, loss_mask]
    columns = [d.astype(jnp.bfloat16) for d in digits] + [old_logp, advantage]
    extra = jnp.pad(jnp.stack(columns, axis=1), ((0, 0), (0, EXTRA - len(columns))))
    own = jnp.concatenate([hidden, extra], axis=1)
    own = gathered(own, NZ, Z)
    own = gathered(own, 4, TOK_VOC, SHORT)
    own = gathered(own, 4, TOK_VOC, LONG)
    other = lax.ppermute(own, TOK_VOC, SWAP)
    half = own.shape[0]
    both = jnp.concatenate([own, other], axis=0)
    hidden_all = both[:, :model]
    small = both[:, model : model + 8].astype(jnp.float32)
    action_all = (small[:, 0] + 128.0 * small[:, 1] + 16384.0 * small[:, 2]).astype(jnp.int32)
    weights, old_all, advant = small[:, 3], small[:, 4], small[:, 5]

    logits = jnp.dot(hidden_all, head_weight, preferred_element_type=jnp.float32)
    first_col = lax.axis_index(TOK_VOC) * width
    columns = first_col + lax.broadcasted_iota(jnp.int32, logits.shape, 1)
    matches = columns == action_all[:, None]
    target_part = jnp.sum(jnp.where(matches, logits, 0.0), axis=1)
    local_top = jnp.max(logits, axis=1)
    shifted = jnp.exp(logits - local_top[:, None])
    stats = jnp.stack(
        [local_top, jnp.sum(shifted, axis=1), jnp.sum(shifted * logits, axis=1), target_part]
    )
    stats = combined(stats, NZ, Z)
    stats = combined(stats, NY, Y)
    turned = lambda s: jnp.where(core == 1, jnp.roll(s, half, axis=1), s)
    top, sumexp, moment, target = turned(combined(turned(stats), NX * NC, (X, C)))

    lse = top + jnp.log(sumexp)
    mean_logit = moment / sumexp
    ratio = jnp.exp(target - lse - old_all)
    clipped = (advant > 0.0) & (ratio > 1.2) | (advant < 0.0) & (ratio < 0.8)
    active = jnp.where(clipped, 0.0, 1.0).astype(jnp.float32)
    policy = -advant * ratio * active * weights
    probability = jnp.exp(logits - lse[:, None])
    onehot = matches.astype(jnp.float32)
    dlogits = policy[:, None] * (onehot - probability) + 0.05 * weights[:, None] * probability * (
        logits - mean_logit[:, None]
    )
    dlogits = dlogits.astype(jnp.bfloat16)

    def to_hidden(d):
        return lax.dot_general(
            d, head_weight, (((1,), (1,)), ((), ())), preferred_element_type=jnp.float32
        )

    theirs = lax.ppermute(to_hidden(dlogits[half:]).astype(jnp.bfloat16), TOK_VOC, SWAP)
    partial = (to_hidden(dlogits[:half]) + theirs.astype(jnp.float32)).astype(jnp.bfloat16)
    partial = scattered(partial, 4, TOK_VOC, LONG).astype(jnp.bfloat16)
    partial = scattered(partial, 4, TOK_VOC, SHORT).astype(jnp.bfloat16)
    grad_hidden = scattered(partial, NZ, Z)
    grad_weight = lax.dot_general(
        hidden_all, dlogits, (((0,), (0,)), ((), ())), preferred_element_type=jnp.float32
    ).astype(jnp.bfloat16)
    return (grad_weight, grad_hidden)


def solution(mesh):
    torus = Mesh(mesh.devices.reshape(NY, NZ, NX, NC), TOK_VOC)
    placed = (P(TOK_VOC, None), P(None, TOK_VOC), P(TOK_VOC), P(TOK_VOC), P(TOK_VOC), P(TOK_VOC))
    return jax.shard_map(
        per_device,
        mesh=torus,
        in_specs=placed,
        out_specs=(P(None, TOK_VOC), P(TOK_VOC, None)),
        check_vma=False,
    )
```

```python
import functools

import jax
import jax.numpy as jnp
from jax import lax
from jax.experimental import pallas as pl
from jax.experimental.pallas import tpu as pltpu
from jax.sharding import Mesh
from jax.sharding import PartitionSpec as P

Y, Z, X, C = "tok_0", "tok_1", "voc_0", "voc_1"
TOK_VOC = (Y, Z, X, C)
NY, NZ, NX, NC = 4, 8, 4, 2
EXTRA = 128
LOGITS_MIB, WEIGHT_MIB = 16, 24


def place(y, z, x, c):
    return ((y % NY) * NZ + z % NZ) * NX * NC + (x % NX) * NC + c % NC


def along_y(core):
    return [[place(y, z, x, core) for y in range(NY)] for z in range(NZ) for x in range(NX)]


def along_x(core):
    return [[place(y, z, x, core) for x in range(NX)] for y in range(NY) for z in range(NZ)]


SHORT = along_x(0) + along_y(1)
CELLS = [(y, z, x, c) for y in range(NY) for z in range(NZ) for x in range(NX) for c in range(NC)]
SWAP = [(place(y, z, x, c), place(y, z, x, 1 - c)) for y, z, x, c in CELLS]


def turn(step, core):
    return [
        (place(y, z, x, c), place(y + step, z, x, c) if c == core else place(y, z, x + step, c))
        for y, z, x, c in CELLS
    ]


TO_LONG = {step: turn(step, 0) for step in (1, 2, 3)}
TO_SHORT = {step: turn(step, 1) for step in (1, 2, 3)}
ORDER = (2, 1, 3)


def exchange(blocks, axis, groups=None):
    return lax.all_to_all(blocks, axis, 0, 0, axis_index_groups=groups)


def gathered(block, count, axis, groups=None):
    whole = exchange(jnp.broadcast_to(block, (count, *block.shape)), axis, groups)
    return whole.reshape(-1, *block.shape[1:])


def total(pieces):
    result = pieces[0].astype(jnp.float32)
    for piece in pieces[1:]:
        result = result + piece.astype(jnp.float32)
    return result


def scattered(partial, count, axis, groups=None):
    pieces = exchange(partial.reshape(count, -1, partial.shape[1]), axis, groups)
    return total([pieces[k] for k in range(count)])


def swapped(value):
    return lax.ppermute(value, TOK_VOC, SWAP)


def merged(pieces):
    top = pieces[0][:, 0]
    for piece in pieces[1:]:
        top = jnp.maximum(top, piece[:, 0])
    scales = [jnp.exp(piece[:, 0] - top) for piece in pieces]
    sumexp = sum(piece[:, 1] * scale for piece, scale in zip(pieces, scales))
    moment = sum(piece[:, 2] * scale for piece, scale in zip(pieces, scales))
    return jnp.stack([top, sumexp, moment, sum(piece[:, 3] for piece in pieces)], axis=1)


def combined(stats):
    pieces = exchange(jnp.broadcast_to(stats, (NZ, *stats.shape)), Z)
    stats = merged([pieces[k] for k in range(NZ)])
    come = {j: lax.ppermute(stats, TOK_VOC, TO_LONG[4 - j]) for j in ORDER}
    stats = merged(
        [stats] + [jnp.concatenate([c[4 - j : 4], c[: 4 - j], c[4:]]) for j, c in come.items()]
    )
    come = {j: lax.ppermute(stats, TOK_VOC, TO_SHORT[4 - j]) for j in ORDER}
    stats = merged(
        [stats] + [jnp.concatenate([c[:4], c[8 - j :], c[4 : 8 - j]]) for j, c in come.items()]
    )
    come = swapped(stats)
    return merged([stats, jnp.concatenate([come[4:], come[:4]])])


def logits_kernel(split, first_ref, *refs):
    pieces, (head, logits, stats) = iter(refs[: sum(split)]), refs[sum(split) :]
    model = head.shape[1]
    for k, count in enumerate(split):
        chunk = jnp.concatenate([next(pieces)[...] for _ in range(count)])
        rows = chunk.shape[0]
        value = lax.dot_general(
            chunk[:, :model],
            head[...],
            (((1,), (1,)), ((), ())),
            preferred_element_type=jnp.float32,
        )
        logits[k * rows : (k + 1) * rows] = value
        small = chunk[:, model:].astype(jnp.float32)
        action = small[:, 0:1] + 128.0 * small[:, 1:2] + 16384.0 * small[:, 2:3]
        column = first_ref[0] + lax.broadcasted_iota(jnp.int32, value.shape, 1)
        match = column == action.astype(jnp.int32)
        top = jnp.max(value, axis=1, keepdims=True)
        shifted = jnp.exp(value - top)
        entries = [
            top,
            jnp.sum(shifted, axis=1, keepdims=True),
            jnp.sum(shifted * value, axis=1, keepdims=True),
            jnp.sum(jnp.where(match, value, 0.0), axis=1, keepdims=True),
            small[:, 4:5],
            small[:, 5:6],
            small[:, 3:4],
            action,
        ]
        lane = lax.broadcasted_iota(jnp.int32, small.shape, 1)
        table = jnp.zeros(small.shape, jnp.float32)
        for at, entry in enumerate(entries):
            table = jnp.where(lane == at, entry, table)
        stats[k] = table.T[: len(entries)]


WHOLE = pl.BlockSpec(memory_space=pltpu.VMEM)
MIB = 1 << 20


def logits_of(chunks, head, first_col):
    split, (width, model) = [len(chunk) for chunk in chunks], head.shape
    count, rows = len(chunks), sum(piece.shape[0] for piece in chunks[0])
    return pl.pallas_call(
        functools.partial(logits_kernel, split),
        in_specs=[pl.BlockSpec(memory_space=pltpu.SMEM)] + [WHOLE] * (sum(split) + 1),
        out_specs=[WHOLE, WHOLE],
        out_shape=[
            jax.ShapeDtypeStruct((count * rows, width), jnp.float32),
            jax.ShapeDtypeStruct((count, 8, rows), jnp.float32),
        ],
        cost_estimate=pl.CostEstimate(
            flops=8 * count * rows * model * width,
            transcendentals=count * rows * width,
            bytes_accessed=2 * (width + count * rows) * model,
        ),
        compiler_params=pltpu.CompilerParams(vmem_limit_bytes=LOGITS_MIB * MIB),
        name="logits",
    )(first_col, *[piece for chunk in chunks for piece in chunk], head)


def weight_kernel(groups, chunks, *refs):
    parts, blocks, (out, padded, turned) = refs[:groups], refs[groups : groups + chunks], refs[-3:]
    at, wide = pl.multiple_of(pl.program_id(0) * out.shape[1], out.shape[1]), out.shape[1]

    @pl.when(pl.program_id(0) == 0)
    def _():
        padded[...] = jnp.zeros_like(padded)
        at = 0
        for part in parts:
            rows, width = part.shape
            padded[at : at + rows, :width] = part[...]
            at += rows
        turned[...] = padded[...].T

    whole = jnp.concatenate([block[:, pl.ds(at, wide)] for block in blocks])
    result = jnp.dot(turned[...], whole, preferred_element_type=jnp.float32)
    out[...] = result[: out.shape[0]].astype(out.dtype)


def head_gradient(dlogits, chunks, model):
    width = dlogits[0].shape[1]
    wide, tokens, block = -(-width // 128) * 128, sum(c.shape[0] for c in chunks), 512
    return pl.pallas_call(
        functools.partial(weight_kernel, len(dlogits), len(chunks)),
        grid=(model // block,),
        in_specs=[WHOLE] * (len(dlogits) + len(chunks)),
        out_specs=pl.BlockSpec((width, block), lambda k: (0, k)),
        out_shape=jax.ShapeDtypeStruct((width, model), jnp.bfloat16),
        scratch_shapes=[
            pltpu.VMEM((tokens, wide), jnp.bfloat16),
            pltpu.VMEM((wide, tokens), jnp.bfloat16),
        ],
        cost_estimate=pl.CostEstimate(
            flops=8 * tokens * model * width,
            transcendentals=0,
            bytes_accessed=2 * (width + tokens) * model,
        ),
        compiler_params=pltpu.CompilerParams(vmem_limit_bytes=WEIGHT_MIB * MIB),
        name="head_gradient",
    )(*dlogits, *chunks)


GROUPS = (((0, 0), (1, 0)), ((0, 1), (0, 3), (1, 1), (1, 3)), ((0, 2), (1, 2)))


def per_device(hidden, head_weight, actions, old_logp, advantage, loss_mask):
    model, width = head_weight.shape
    head = head_weight.T
    digits = [actions % 128, (actions // 128) % 128, actions // 16384, loss_mask]
    columns = [d.astype(jnp.bfloat16) for d in digits] + [old_logp, advantage]
    extra = jnp.pad(jnp.stack(columns, axis=1), ((0, 0), (0, EXTRA - len(columns))))
    block = jnp.concatenate([hidden, extra], axis=1)
    block = gathered(block, NZ, Z)
    block = gathered(block, 4, TOK_VOC, SHORT)
    rows, back, ahead = block.shape[0], TO_LONG[3], TO_LONG[1]
    first_col = lax.axis_index(TOK_VOC) * width
    logits, table, chunks = {}, {}, {}

    def worked(group):
        part, lines = logits_of([chunks[c] for c in group], head, first_col.reshape(1))
        logits[group] = part
        table.update({c: lines[k] for k, c in enumerate(group)})
        return part

    near = [lax.ppermute(block, TOK_VOC, back), lax.ppermute(block, TOK_VOC, ahead)]
    chunks[0, 0], chunks[1, 0] = [block], [swapped(block)]
    near, _ = lax.optimization_barrier((near, worked(GROUPS[0])))
    far = [
        lax.ppermute(near[0][: rows // 2], TOK_VOC, back),
        lax.ppermute(near[1][rows // 2 :], TOK_VOC, ahead),
    ]
    for j, chunk in zip((1, 3), near):
        chunks[0, j], chunks[1, j] = [chunk], [swapped(chunk)]
    far, _ = lax.optimization_barrier((far, worked(GROUPS[1])))
    chunks[0, 2], chunks[1, 2] = far, [swapped(piece) for piece in far]
    worked(GROUPS[2])
    table = jnp.stack([table[half, j] for half in range(2) for j in range(4)])
    stats, rest = combined(table[:, :4]), table[:, 4:]
    top, sumexp, moment, target = [stats[:, k] for k in range(4)]
    old_all, advant, weights, action = [rest[:, k] for k in range(4)]
    lse = top + jnp.log(sumexp)
    mean_logit = moment / sumexp
    ratio = jnp.exp(target - lse - old_all)
    clipped = (advant > 0.0) & (ratio > 1.2) | (advant < 0.0) & (ratio < 0.8)
    active = jnp.where(clipped, 0.0, 1.0).astype(jnp.float32)
    policy = -advant * ratio * active * weights
    entropy = 0.05 * weights
    action = action.astype(jnp.int32)

    dlogits, piece = {}, {}
    for group in GROUPS:
        value = logits[group]
        of = lambda a: jnp.concatenate([a[4 * half + j] for half, j in group])[:, None]
        match = first_col + lax.broadcasted_iota(jnp.int32, value.shape, 1) == of(action)
        probability = jnp.exp(value - of(lse))
        d = of(policy) * (match.astype(jnp.float32) - probability)
        d = d + of(entropy) * probability * (value - of(mean_logit))
        dlogits[group] = d.astype(jnp.bfloat16)
        piece.update({c: dlogits[group][k * rows : (k + 1) * rows] for k, c in enumerate(group)})

    def to_hidden(d):
        return jnp.dot(d, head, preferred_element_type=jnp.float32)

    theirs = {j: swapped(to_hidden(piece[1, j]).astype(jnp.bfloat16)) for j in (*ORDER, 0)}

    def summed(j, *more):
        return total([to_hidden(piece[0, j]), theirs[j], *more])

    far = summed(2).astype(jnp.bfloat16)
    up = jnp.pad(lax.ppermute(far[: rows // 2], TOK_VOC, ahead), ((0, rows // 2), (0, 0)))
    down = jnp.pad(lax.ppermute(far[rows // 2 :], TOK_VOC, back), ((rows // 2, 0), (0, 0)))
    leaving = [summed(1, up).astype(jnp.bfloat16), summed(3, down).astype(jnp.bfloat16)]
    come = [lax.ppermute(leaving[0], TOK_VOC, ahead), lax.ppermute(leaving[1], TOK_VOC, back)]
    partial = summed(0)

    ready, _ = lax.optimization_barrier(([dlogits[group] for group in GROUPS], leaving))
    grad_weight = head_gradient(ready, [p for group in GROUPS for c in group for p in chunks[c]], model)
    grad_weight, come = lax.optimization_barrier((grad_weight, come))

    partial = total([partial, *come]).astype(jnp.bfloat16)
    partial = scattered(partial, 4, TOK_VOC, SHORT).astype(jnp.bfloat16)
    grad_hidden = scattered(partial, NZ, Z)
    return (grad_weight.T, grad_hidden)


def solution(mesh):
    torus = Mesh(mesh.devices.reshape(NY, NZ, NX, NC), TOK_VOC)
    placed = (P(TOK_VOC, None), P(None, TOK_VOC), P(TOK_VOC), P(TOK_VOC), P(TOK_VOC), P(TOK_VOC))
    return jax.shard_map(
        per_device,
        mesh=torus,
        in_specs=placed,
        out_specs=(P(None, TOK_VOC), P(TOK_VOC, None)),
        check_vma=False,
    )
```

```python
import functools

import jax
import jax.numpy as jnp
from jax import lax
from jax.experimental import pallas as pl
from jax.experimental.pallas import tpu as pltpu
from jax.sharding import Mesh
from jax.sharding import PartitionSpec as P

Y, Z, X, C = "tok_0", "tok_1", "voc_0", "voc_1"
TOK_VOC = (Y, Z, X, C)
NY, NZ, NX, NC = 4, 8, 4, 2
EXTRA = 128
LOGITS_MIB, WEIGHT_MIB, SMALL_MIB = 12, 12, 4


def place(y, z, x, c):
    return ((y % NY) * NZ + z % NZ) * NX * NC + (x % NX) * NC + c % NC


CELLS = [(y, z, x, c) for y in range(NY) for z in range(NZ) for x in range(NX) for c in range(NC)]
SWAP = [(place(y, z, x, c), place(y, z, x, 1 - c)) for y, z, x, c in CELLS]


def turn(step, core):
    return [
        (place(y, z, x, c), place(y + step, z, x, c) if c == core else place(y, z, x + step, c))
        for y, z, x, c in CELLS
    ]


TO_LONG = {step: turn(step, 0) for step in (1, 2, 3)}
TO_SHORT = {step: turn(step, 1) for step in (1, 2, 3)}
ORDER = (2, 1, 3)


def exchange(blocks, axis):
    return lax.all_to_all(blocks, axis, 0, 0)


def gathered(block, count, axis):
    whole = exchange(jnp.broadcast_to(block, (count, *block.shape)), axis)
    return whole.reshape(-1, *block.shape[1:])


def total(pieces):
    result = pieces[0].astype(jnp.float32)
    for piece in pieces[1:]:
        result = result + piece.astype(jnp.float32)
    return result


def scattered(partial, count, axis):
    pieces = exchange(partial.reshape(count, -1, partial.shape[1]), axis)
    return total([pieces[k] for k in range(count)])


def swapped(value):
    return lax.ppermute(value, TOK_VOC, SWAP)


def merged(pieces):
    top = pieces[0][:, 0]
    for piece in pieces[1:]:
        top = jnp.maximum(top, piece[:, 0])
    scales = [jnp.exp(piece[:, 0] - top) for piece in pieces]
    sumexp = sum(piece[:, 1] * scale for piece, scale in zip(pieces, scales))
    moment = sum(piece[:, 2] * scale for piece, scale in zip(pieces, scales))
    return jnp.stack([top, sumexp, moment, sum(piece[:, 3] for piece in pieces)], axis=1)


def combined(stats):
    pieces = exchange(jnp.broadcast_to(stats, (NZ, *stats.shape)), Z)
    stats = merged([pieces[k] for k in range(NZ)])
    come = {j: lax.ppermute(stats, TOK_VOC, TO_LONG[4 - j]) for j in ORDER}
    stats = merged(
        [stats] + [jnp.concatenate([c[4 - j : 4], c[: 4 - j], c[4:]]) for j, c in come.items()]
    )
    come = {j: lax.ppermute(stats, TOK_VOC, TO_SHORT[4 - j]) for j in ORDER}
    stats = merged(
        [stats] + [jnp.concatenate([c[:4], c[8 - j :], c[4 : 8 - j]]) for j, c in come.items()]
    )
    come = swapped(stats)
    return merged([stats, jnp.concatenate([come[4:], come[:4]])])


def logits_kernel(split, first_ref, *refs):
    pieces, (head, logits, stats) = refs[: sum(split)], refs[sum(split) :]
    model, rows = head.shape[1], stats.shape[2]
    whole = jnp.concatenate([piece[...] for piece in pieces])
    logits[...] = lax.dot_general(
        whole[:, :model], head[...], (((1,), (1,)), ((), ())), preferred_element_type=jnp.float32
    )
    for k in range(len(split)):
        value, chunk = logits[k * rows : (k + 1) * rows], whole[k * rows : (k + 1) * rows]
        small = chunk[:, model:].astype(jnp.float32)
        action = small[:, 0:1] + 128.0 * small[:, 1:2] + 16384.0 * small[:, 2:3]
        column = first_ref[0] + lax.broadcasted_iota(jnp.int32, value.shape, 1)
        match = column == action.astype(jnp.int32)
        top = jnp.max(value, axis=1, keepdims=True)
        shifted = jnp.exp(value - top)
        entries = [
            top,
            jnp.sum(shifted, axis=1, keepdims=True),
            jnp.sum(shifted * value, axis=1, keepdims=True),
            jnp.sum(jnp.where(match, value, 0.0), axis=1, keepdims=True),
            small[:, 4:5],
            small[:, 5:6],
            small[:, 3:4],
            action,
        ]
        lane = lax.broadcasted_iota(jnp.int32, small.shape, 1)
        table = jnp.zeros(small.shape, jnp.float32)
        for at, entry in enumerate(entries):
            table = jnp.where(lane == at, entry, table)
        stats[k] = table.T[: len(entries)]


def place_kernel(at_ref, *refs):
    *blocks, out = refs
    rows = blocks[0].shape[0]
    for j, block in enumerate(blocks):
        start = pl.multiple_of(lax.rem(at_ref[0] + j, len(blocks)) * rows, rows)
        out[pl.ds(start, rows), :] = block[...]


def placed(blocks, at):
    rows, columns = blocks[0].shape
    return pl.pallas_call(
        place_kernel,
        in_specs=[pl.BlockSpec(memory_space=pltpu.SMEM)] + [WHOLE] * len(blocks),
        out_specs=WHOLE,
        out_shape=jax.ShapeDtypeStruct((len(blocks) * rows, columns), blocks[0].dtype),
        compiler_params=pltpu.CompilerParams(vmem_limit_bytes=SMALL_MIB * MIB),
        name="placed",
    )(at.reshape(1), *blocks)


def split_kernel(parts, at_ref, *refs):
    terms, outs = refs[:parts], refs[parts:]
    rows = outs[0].shape[0]
    for j, out in enumerate(outs):
        start = pl.multiple_of(lax.rem(at_ref[0] + j, len(outs)) * rows, rows)
        out[...] = total([term[pl.ds(start, rows), :] for term in terms]).astype(out.dtype)


def split_total(terms, count, at):
    rows, columns = terms[0].shape
    piece = jax.ShapeDtypeStruct((rows // count, columns), jnp.bfloat16)
    return pl.pallas_call(
        functools.partial(split_kernel, len(terms)),
        in_specs=[pl.BlockSpec(memory_space=pltpu.SMEM)] + [WHOLE] * len(terms),
        out_specs=[WHOLE] * count,
        out_shape=[piece] * count,
        compiler_params=pltpu.CompilerParams(vmem_limit_bytes=SMALL_MIB * MIB),
        name="split_total",
    )(at.reshape(1), *terms)


WHOLE = pl.BlockSpec(memory_space=pltpu.VMEM)
MIB = 1 << 20


def logits_of(chunks, head, first_col):
    split, (width, model) = [len(chunk) for chunk in chunks], head.shape
    count, rows = len(chunks), sum(piece.shape[0] for piece in chunks[0])
    return pl.pallas_call(
        functools.partial(logits_kernel, split),
        in_specs=[pl.BlockSpec(memory_space=pltpu.SMEM)] + [WHOLE] * (sum(split) + 1),
        out_specs=[WHOLE, WHOLE],
        out_shape=[
            jax.ShapeDtypeStruct((count * rows, width), jnp.float32),
            jax.ShapeDtypeStruct((count, 8, rows), jnp.float32),
        ],
        cost_estimate=pl.CostEstimate(
            flops=8 * count * rows * model * width,
            transcendentals=count * rows * width,
            bytes_accessed=2 * (width + count * rows) * model,
        ),
        compiler_params=pltpu.CompilerParams(vmem_limit_bytes=LOGITS_MIB * MIB),
        name="logits",
    )(first_col, *[piece for chunk in chunks for piece in chunk], head)


def weight_kernel(groups, chunks, *refs):
    parts, blocks, (out, padded, turned) = refs[:groups], refs[groups : groups + chunks], refs[-3:]
    at, wide = pl.multiple_of(pl.program_id(0) * out.shape[1], out.shape[1]), out.shape[1]

    @pl.when(pl.program_id(0) == 0)
    def _():
        padded[...] = jnp.zeros_like(padded)
        at = 0
        for part in parts:
            rows, width = part.shape
            padded[at : at + rows, :width] = part[...]
            at += rows
        turned[...] = padded[...].T

    whole = jnp.concatenate([block[:, pl.ds(at, wide)] for block in blocks])
    result = jnp.dot(turned[...], whole, preferred_element_type=jnp.float32)
    out[...] = result[: out.shape[0]].astype(out.dtype)


def head_gradient(dlogits, chunks, model):
    width = dlogits[0].shape[1]
    wide, tokens, block = -(-width // 128) * 128, sum(c.shape[0] for c in chunks), 512
    return pl.pallas_call(
        functools.partial(weight_kernel, len(dlogits), len(chunks)),
        grid=(model // block,),
        in_specs=[WHOLE] * (len(dlogits) + len(chunks)),
        out_specs=pl.BlockSpec((width, block), lambda k: (0, k)),
        out_shape=jax.ShapeDtypeStruct((width, model), jnp.bfloat16),
        scratch_shapes=[
            pltpu.VMEM((tokens, wide), jnp.bfloat16),
            pltpu.VMEM((wide, tokens), jnp.bfloat16),
        ],
        cost_estimate=pl.CostEstimate(
            flops=8 * tokens * model * width,
            transcendentals=0,
            bytes_accessed=2 * (width + tokens) * model,
        ),
        compiler_params=pltpu.CompilerParams(vmem_limit_bytes=WEIGHT_MIB * MIB),
        name="head_gradient",
    )(*dlogits, *chunks)


GROUPS = (((0, 0), (1, 0)), ((0, 1), (0, 3), (1, 1), (1, 3)), ((0, 2), (1, 2)))


def per_device(hidden, head_weight, actions, old_logp, advantage, loss_mask):
    model, width = head_weight.shape
    head = head_weight.T
    digits = [actions % 128, (actions // 128) % 128, actions // 16384, loss_mask]
    columns = [d.astype(jnp.bfloat16) for d in digits] + [old_logp, advantage]
    extra = jnp.pad(jnp.stack(columns, axis=1), ((0, 0), (0, EXTRA - len(columns))))
    block = jnp.concatenate([hidden, extra], axis=1)
    block = gathered(block, NZ, Z)
    place_short = jnp.where(lax.axis_index(C) == 0, lax.axis_index(X), lax.axis_index(Y))
    block = placed(
        [block] + [lax.ppermute(block, TOK_VOC, TO_SHORT[4 - j]) for j in (1, 2, 3)], place_short
    )
    rows, back, ahead = block.shape[0], TO_LONG[3], TO_LONG[1]
    first_col = lax.axis_index(TOK_VOC) * width
    logits, table, chunks = {}, {}, {}

    def worked(group):
        part, lines = logits_of([chunks[c] for c in group], head, first_col.reshape(1))
        logits[group] = part
        table.update({c: lines[k] for k, c in enumerate(group)})
        return part

    near = [lax.ppermute(block, TOK_VOC, back), lax.ppermute(block, TOK_VOC, ahead)]
    chunks[0, 0], chunks[1, 0] = [block], [swapped(block)]
    near, _ = lax.optimization_barrier((near, worked(GROUPS[0])))
    far = [
        lax.ppermute(near[0][: rows // 2], TOK_VOC, back),
        lax.ppermute(near[1][rows // 2 :], TOK_VOC, ahead),
    ]
    for j, chunk in zip((1, 3), near):
        chunks[0, j], chunks[1, j] = [chunk], [swapped(chunk)]
    far, _ = lax.optimization_barrier((far, worked(GROUPS[1])))
    chunks[0, 2], chunks[1, 2] = far, [swapped(piece) for piece in far]
    worked(GROUPS[2])
    table = jnp.stack([table[half, j] for half in range(2) for j in range(4)])
    stats, rest = combined(table[:, :4]), table[:, 4:]
    top, sumexp, moment, target = [stats[:, k] for k in range(4)]
    old_all, advant, weights, action = [rest[:, k] for k in range(4)]
    lse = top + jnp.log(sumexp)
    mean_logit = moment / sumexp
    ratio = jnp.exp(target - lse - old_all)
    clipped = (advant > 0.0) & (ratio > 1.2) | (advant < 0.0) & (ratio < 0.8)
    active = jnp.where(clipped, 0.0, 1.0).astype(jnp.float32)
    policy = -advant * ratio * active * weights
    entropy = 0.05 * weights
    action = action.astype(jnp.int32)

    dlogits, piece = {}, {}
    for group in GROUPS:
        value = logits[group]
        of = lambda a: jnp.concatenate([a[4 * half + j] for half, j in group])[:, None]
        match = first_col + lax.broadcasted_iota(jnp.int32, value.shape, 1) == of(action)
        probability = jnp.exp(value - of(lse))
        d = of(policy) * (match.astype(jnp.float32) - probability)
        d = d + of(entropy) * probability * (value - of(mean_logit))
        dlogits[group] = d.astype(jnp.bfloat16)
        piece.update({c: dlogits[group][k * rows : (k + 1) * rows] for k, c in enumerate(group)})

    def to_hidden(d):
        return jnp.dot(d, head, preferred_element_type=jnp.float32)

    def theirs(d):
        return swapped(to_hidden(d).astype(jnp.bfloat16))

    theirs_far, theirs_near = theirs(piece[1, 2]), theirs(dlogits[GROUPS[1]][2 * rows :])
    far = total([to_hidden(piece[0, 2]), theirs_far]).astype(jnp.bfloat16)
    up = jnp.pad(lax.ppermute(far[: rows // 2], TOK_VOC, ahead), ((0, rows // 2), (0, 0)))
    down = jnp.pad(lax.ppermute(far[rows // 2 :], TOK_VOC, back), ((rows // 2, 0), (0, 0)))
    leaving = [
        total([to_hidden(piece[0, 1]), theirs_near[:rows], up]).astype(jnp.bfloat16),
        total([to_hidden(piece[0, 3]), theirs_near[rows:], down]).astype(jnp.bfloat16),
    ]
    come = [lax.ppermute(leaving[0], TOK_VOC, ahead), lax.ppermute(leaving[1], TOK_VOC, back)]
    kept, _ = lax.optimization_barrier((dlogits[GROUPS[0]], far))
    terms = [to_hidden(kept[:rows]), theirs(kept[rows:])]

    ready, _ = lax.optimization_barrier(([dlogits[group] for group in GROUPS], leaving))
    grad_weight = head_gradient(ready, [p for group in GROUPS for c in group for p in chunks[c]], model)
    grad_weight, come = lax.optimization_barrier((grad_weight, come))

    pieces = split_total([*terms, *come], 4, place_short)
    come = [lax.ppermute(pieces[j], TOK_VOC, TO_SHORT[j]) for j in (1, 2, 3)]
    partial = total([pieces[0], *come]).astype(jnp.bfloat16)
    grad_hidden = scattered(partial, NZ, Z)
    return (grad_weight.T, grad_hidden)


def solution(mesh):
    torus = Mesh(mesh.devices.reshape(NY, NZ, NX, NC), TOK_VOC)
    placed = (P(TOK_VOC, None), P(None, TOK_VOC), P(TOK_VOC), P(TOK_VOC), P(TOK_VOC), P(TOK_VOC))
    return jax.shard_map(
        per_device,
        mesh=torus,
        in_specs=placed,
        out_specs=(P(None, TOK_VOC), P(TOK_VOC, None)),
        check_vma=False,
    )
```

```python
import functools

import jax
import jax.numpy as jnp
from jax import lax
from jax.experimental import pallas as pl
from jax.experimental.pallas import tpu as pltpu
from jax.sharding import Mesh
from jax.sharding import PartitionSpec as P


Y, Z, X, C = "tok_0", "tok_1", "voc_0", "voc_1"
TOK_VOC = (Y, Z, X, C)
NY, NZ, NX, NC = 4, 8, 4, 2
EXTRA = 128
LOGITS_MIB, WEIGHT_MIB, SMALL_MIB = 12, 12, 4


def place(y, z, x, c):
    return ((y % NY) * NZ + z % NZ) * NX * NC + (x % NX) * NC + c % NC


CELLS = [(y, z, x, c) for y in range(NY) for z in range(NZ) for x in range(NX) for c in range(NC)]
SWAP = [(place(y, z, x, c), place(y, z, x, 1 - c)) for y, z, x, c in CELLS]


def turn(step, core):
    return [
        (place(y, z, x, c), place(y + step, z, x, c) if c == core else place(y, z, x + step, c))
        for y, z, x, c in CELLS
    ]


TO_LONG = {step: turn(step, 0) for step in (1, 2, 3)}
TO_SHORT = {step: turn(step, 1) for step in (1, 2, 3)}
ORDER = (2, 1, 3)


def exchange(blocks, axis):
    return lax.all_to_all(blocks, axis, 0, 0)


def gathered(block, count, axis):
    whole = exchange(jnp.broadcast_to(block, (count, *block.shape)), axis)
    return whole.reshape(-1, *block.shape[1:])


def total(pieces):
    result = pieces[0].astype(jnp.float32)
    for piece in pieces[1:]:
        result = result + piece.astype(jnp.float32)
    return result


def scattered(partial, count, axis):
    pieces = exchange(partial.reshape(count, -1, partial.shape[1]), axis)
    return total([pieces[k] for k in range(count)])


def sent(value, table, step):
    return lax.ppermute(value, TOK_VOC, table[step])


def swapped(value):
    return lax.ppermute(value, TOK_VOC, SWAP)


def merged(pieces):
    top = pieces[0][:, 0]
    for piece in pieces[1:]:
        top = jnp.maximum(top, piece[:, 0])
    scales = [jnp.exp(piece[:, 0] - top) for piece in pieces]
    sumexp = sum(piece[:, 1] * scale for piece, scale in zip(pieces, scales))
    moment = sum(piece[:, 2] * scale for piece, scale in zip(pieces, scales))
    return jnp.stack([top, sumexp, moment, sum(piece[:, 3] for piece in pieces)], axis=1)


def combined(stats):
    pieces = exchange(jnp.broadcast_to(stats, (NZ, *stats.shape)), Z)
    stats = merged([pieces[k] for k in range(NZ)])
    come = {j: sent(stats, TO_LONG, 4 - j) for j in ORDER}
    stats = merged(
        [stats] + [jnp.concatenate([c[4 - j : 4], c[: 4 - j], c[4:]]) for j, c in come.items()]
    )
    come = {j: sent(stats, TO_SHORT, 4 - j) for j in ORDER}
    stats = merged(
        [stats] + [jnp.concatenate([c[:4], c[8 - j :], c[4 : 8 - j]]) for j, c in come.items()]
    )
    come = swapped(stats)
    return merged([stats, jnp.concatenate([come[4:], come[:4]])])


def logits_kernel(split, first_ref, *refs):
    pieces, (head, logits, stats) = refs[: sum(split)], refs[sum(split) :]
    model, rows = head.shape[1], stats.shape[2]
    whole = jnp.concatenate([piece[...] for piece in pieces])
    logits[...] = lax.dot_general(
        whole[:, :model], head[...], (((1,), (1,)), ((), ())), preferred_element_type=jnp.float32
    )
    for k in range(len(split)):
        value, chunk = logits[k * rows : (k + 1) * rows], whole[k * rows : (k + 1) * rows]
        small = chunk[:, model:].astype(jnp.float32)
        action = small[:, 0:1] + 128.0 * small[:, 1:2] + 16384.0 * small[:, 2:3]
        column = first_ref[0] + lax.broadcasted_iota(jnp.int32, value.shape, 1)
        match = column == action.astype(jnp.int32)
        top = jnp.max(value, axis=1, keepdims=True)
        shifted = jnp.exp(value - top)
        entries = [
            top,
            jnp.sum(shifted, axis=1, keepdims=True),
            jnp.sum(shifted * value, axis=1, keepdims=True),
            jnp.sum(jnp.where(match, value, 0.0), axis=1, keepdims=True),
            small[:, 4:5],
            small[:, 5:6],
            small[:, 3:4],
            action,
        ]
        lane = lax.broadcasted_iota(jnp.int32, small.shape, 1)
        table = jnp.zeros(small.shape, jnp.float32)
        for at, entry in enumerate(entries):
            table = jnp.where(lane == at, entry, table)
        stats[k] = table.T[: len(entries)]


def place_kernel(at_ref, *refs):
    *blocks, out = refs
    rows = blocks[0].shape[0]
    for j, block in enumerate(blocks):
        start = pl.multiple_of(lax.rem(at_ref[0] + j, len(blocks)) * rows, rows)
        out[pl.ds(start, rows), :] = block[...]


def placed(blocks, at):
    rows, columns = blocks[0].shape
    return pl.pallas_call(
        place_kernel,
        in_specs=[pl.BlockSpec(memory_space=pltpu.SMEM)] + [WHOLE] * len(blocks),
        out_specs=WHOLE,
        out_shape=jax.ShapeDtypeStruct((len(blocks) * rows, columns), blocks[0].dtype),
        compiler_params=pltpu.CompilerParams(vmem_limit_bytes=SMALL_MIB * MIB),
        name="placed",
    )(at.reshape(1), *blocks)


def split_kernel(parts, at_ref, *refs):
    terms, outs = refs[:parts], refs[parts:]
    rows = outs[0].shape[0]
    for j, out in enumerate(outs):
        start = pl.multiple_of(lax.rem(at_ref[0] + j, len(outs)) * rows, rows)
        out[...] = total([term[pl.ds(start, rows), :] for term in terms]).astype(out.dtype)


def split_total(terms, count, at):
    rows, columns = terms[0].shape
    piece = jax.ShapeDtypeStruct((rows // count, columns), jnp.bfloat16)
    return pl.pallas_call(
        functools.partial(split_kernel, len(terms)),
        in_specs=[pl.BlockSpec(memory_space=pltpu.SMEM)] + [WHOLE] * len(terms),
        out_specs=[WHOLE] * count,
        out_shape=[piece] * count,
        compiler_params=pltpu.CompilerParams(vmem_limit_bytes=SMALL_MIB * MIB),
        name="split_total",
    )(at.reshape(1), *terms)


WHOLE = pl.BlockSpec(memory_space=pltpu.VMEM)
MIB = 1 << 20


def logits_of(chunks, head, first_col):
    split, (width, model) = [len(chunk) for chunk in chunks], head.shape
    count, rows = len(chunks), sum(piece.shape[0] for piece in chunks[0])
    return pl.pallas_call(
        functools.partial(logits_kernel, split),
        in_specs=[pl.BlockSpec(memory_space=pltpu.SMEM)] + [WHOLE] * (sum(split) + 1),
        out_specs=[WHOLE, WHOLE],
        out_shape=[
            jax.ShapeDtypeStruct((count * rows, width), jnp.float32),
            jax.ShapeDtypeStruct((count, 8, rows), jnp.float32),
        ],
        cost_estimate=pl.CostEstimate(
            flops=8 * count * rows * model * width,
            transcendentals=count * rows * width,
            bytes_accessed=2 * (width + count * rows) * model,
        ),
        compiler_params=pltpu.CompilerParams(vmem_limit_bytes=LOGITS_MIB * MIB),
        name="logits",
    )(first_col, *[piece for chunk in chunks for piece in chunk], head)


def weight_kernel(groups, chunks, *refs):
    parts, blocks, (out, padded, turned) = refs[:groups], refs[groups : groups + chunks], refs[-3:]
    at, wide = pl.multiple_of(pl.program_id(0) * out.shape[1], out.shape[1]), out.shape[1]

    @pl.when(pl.program_id(0) == 0)
    def _():
        padded[...] = jnp.zeros_like(padded)
        at = 0
        for part in parts:
            rows, width = part.shape
            padded[at : at + rows, :width] = part[...]
            at += rows
        turned[...] = padded[...].T

    whole = jnp.concatenate([block[:, pl.ds(at, wide)] for block in blocks])
    result = jnp.dot(turned[...], whole, preferred_element_type=jnp.float32)
    out[...] = result[: out.shape[0]].astype(out.dtype)


def head_gradient(dlogits, chunks, model):
    width = dlogits[0].shape[1]
    wide, tokens, block = -(-width // 128) * 128, sum(c.shape[0] for c in chunks), 512
    return pl.pallas_call(
        functools.partial(weight_kernel, len(dlogits), len(chunks)),
        grid=(model // block,),
        in_specs=[WHOLE] * (len(dlogits) + len(chunks)),
        out_specs=pl.BlockSpec((width, block), lambda k: (0, k)),
        out_shape=jax.ShapeDtypeStruct((width, model), jnp.bfloat16),
        scratch_shapes=[
            pltpu.VMEM((tokens, wide), jnp.bfloat16),
            pltpu.VMEM((wide, tokens), jnp.bfloat16),
        ],
        cost_estimate=pl.CostEstimate(
            flops=8 * tokens * model * width,
            transcendentals=0,
            bytes_accessed=2 * (width + tokens) * model,
        ),
        compiler_params=pltpu.CompilerParams(vmem_limit_bytes=WEIGHT_MIB * MIB),
        name="head_gradient",
    )(*dlogits, *chunks)


GROUPS = (((0, 0), (1, 0)), ((0, 1), (0, 3), (1, 1), (1, 3)), ((0, 2), (1, 2)))


def per_device(hidden, head_weight, actions, old_logp, advantage, loss_mask):
    model, width = head_weight.shape
    head = head_weight.T
    digits = [actions % 128, (actions // 128) % 128, actions // 16384, loss_mask]
    columns = [d.astype(jnp.bfloat16) for d in digits] + [old_logp, advantage]
    extra = jnp.pad(jnp.stack(columns, axis=1), ((0, 0), (0, EXTRA - len(columns))))
    block = jnp.concatenate([hidden, extra], axis=1)
    block = gathered(block, NZ, Z)
    place_short = jnp.where(lax.axis_index(C) == 0, lax.axis_index(X), lax.axis_index(Y))
    block = placed([block] + [sent(block, TO_SHORT, 4 - j) for j in (1, 2, 3)], place_short)
    rows = block.shape[0]
    first_col = lax.axis_index(TOK_VOC) * width
    logits, table, chunks = {}, {}, {}

    def worked(group):
        part, lines = logits_of([chunks[c] for c in group], head, first_col.reshape(1))
        logits[group] = part
        table.update({c: lines[k] for k, c in enumerate(group)})
        return part

    near = [sent(block, TO_LONG, 3), sent(block, TO_LONG, 1)]
    chunks[0, 0], chunks[1, 0] = [block], [swapped(block)]
    near, _ = lax.optimization_barrier((near, worked(GROUPS[0])))
    far = [sent(near[0][: rows // 2], TO_LONG, 3), sent(near[1][rows // 2 :], TO_LONG, 1)]
    for j, chunk in zip((1, 3), near):
        chunks[0, j], chunks[1, j] = [chunk], [swapped(chunk)]
    far, _ = lax.optimization_barrier((far, worked(GROUPS[1])))
    chunks[0, 2], chunks[1, 2] = far, [swapped(piece) for piece in far]
    worked(GROUPS[2])
    table = jnp.stack([table[half, j] for half in range(2) for j in range(4)])
    stats, rest = combined(table[:, :4]), table[:, 4:]
    top, sumexp, moment, target = [stats[:, k] for k in range(4)]
    old_all, advant, weights, action = [rest[:, k] for k in range(4)]
    lse = top + jnp.log(sumexp)
    mean_logit = moment / sumexp
    ratio = jnp.exp(target - lse - old_all)
    clipped = (advant > 0.0) & (ratio > 1.2) | (advant < 0.0) & (ratio < 0.8)
    active = jnp.where(clipped, 0.0, 1.0).astype(jnp.float32)
    policy = -advant * ratio * active * weights
    entropy = 0.05 * weights
    action = action.astype(jnp.int32)

    dlogits, piece = {}, {}
    for group in GROUPS:
        value = logits[group]
        of = lambda a: jnp.concatenate([a[4 * half + j] for half, j in group])[:, None]
        match = first_col + lax.broadcasted_iota(jnp.int32, value.shape, 1) == of(action)
        probability = jnp.exp(value - of(lse))
        d = of(policy) * (match.astype(jnp.float32) - probability)
        d = d + of(entropy) * probability * (value - of(mean_logit))
        dlogits[group] = d.astype(jnp.bfloat16)
        piece.update({c: dlogits[group][k * rows : (k + 1) * rows] for k, c in enumerate(group)})

    def to_hidden(d):
        return jnp.dot(d, head, preferred_element_type=jnp.float32)

    def theirs(d):
        return swapped(to_hidden(d).astype(jnp.bfloat16))

    theirs_far, theirs_near = theirs(piece[1, 2]), theirs(dlogits[GROUPS[1]][2 * rows :])
    far = total([to_hidden(piece[0, 2]), theirs_far]).astype(jnp.bfloat16)
    up = jnp.pad(sent(far[: rows // 2], TO_LONG, 1), ((0, rows // 2), (0, 0)))
    down = jnp.pad(sent(far[rows // 2 :], TO_LONG, 3), ((rows // 2, 0), (0, 0)))
    leaving = [
        total([to_hidden(piece[0, 1]), theirs_near[:rows], up]).astype(jnp.bfloat16),
        total([to_hidden(piece[0, 3]), theirs_near[rows:], down]).astype(jnp.bfloat16),
    ]
    come = [sent(leaving[0], TO_LONG, 1), sent(leaving[1], TO_LONG, 3)]
    kept, _ = lax.optimization_barrier((dlogits[GROUPS[0]], far))
    terms = [to_hidden(kept[:rows]), theirs(kept[rows:])]

    ready, _ = lax.optimization_barrier(([dlogits[group] for group in GROUPS], leaving))
    grad_weight = head_gradient(ready, [p for group in GROUPS for c in group for p in chunks[c]], model)
    grad_weight, come = lax.optimization_barrier((grad_weight, come))

    pieces = split_total([*terms, *come], 4, place_short)
    come = [sent(pieces[j], TO_SHORT, j) for j in (1, 2, 3)]
    partial = total([pieces[0], *come]).astype(jnp.bfloat16)
    grad_hidden = scattered(partial, NZ, Z)
    return (grad_weight.T, grad_hidden)


def solution(mesh):
    torus = Mesh(mesh.devices.reshape(NY, NZ, NX, NC), TOK_VOC)
    placed = (P(TOK_VOC, None), P(None, TOK_VOC), P(TOK_VOC), P(TOK_VOC), P(TOK_VOC), P(TOK_VOC))
    return jax.shard_map(
        per_device,
        mesh=torus,
        in_specs=placed,
        out_specs=(P(None, TOK_VOC), P(TOK_VOC, None)),
        check_vma=False,
    )
```
